32 devices in a mesh: rep: 1 (over z), dp: 32 (over x, y, core).
Axes of the slice: x: 4, y: 4, z: 1, core: 2. Of those that a mesh axis runs over, the one named last changes fastest.
The devices are a block of a 4x4x8 slice.
Arguments:
- g_w_gate: bfloat16 [32, 2, 896, 4864], P(('rep', 'dp'))
- g_w_up: bfloat16 [32, 2, 896, 4864], P(('rep', 'dp'))
- g_w_down: bfloat16 [32, 2, 4864, 896], P(('rep', 'dp'))
- w_gate: bfloat16 [2, 896, 4864], replicated
- w_up: bfloat16 [2, 896, 4864], replicated
- w_down: bfloat16 [2, 4864, 896], replicated
- m_w_gate: float32 [2, 896, 4864], P(None, 'dp')
- m_w_up: float32 [2, 896, 4864], P(None, 'dp')
- m_w_down: float32 [2, 4864, 896], P(None, 'dp')
- v_w_gate: float32 [2, 896, 4864], P(None, 'dp')
- v_w_up: float32 [2, 896, 4864], P(None, 'dp')
- v_w_down: float32 [2, 4864, 896], P(None, 'dp')
Outputs:
- output 1: bfloat16 [2, 896, 4864], P('rep')
- output 2: bfloat16 [2, 896, 4864], P('rep')
- output 3: bfloat16 [2, 4864, 896], P('rep')
- output 4: float32 [2, 896, 4864], P('rep', 'dp')
- output 5: float32 [2, 896, 4864], P('rep', 'dp')
- output 6: float32 [2, 4864, 896], P('rep', 'dp')
- output 7: float32 [2, 896, 4864], P('rep', 'dp')
- output 8: float32 [2, 896, 4864], P('rep', 'dp')
- output 9: float32 [2, 4864, 896], P('rep', 'dp')
All inputs are finite; a program needn't handle non-finite values.
Results may differ from the reference program's by a relative error of at most 0.022.
Values are sent between devices in bfloat16 or wider.
A program may use at most 768 MiB of HBM per device.

```python
import jax
import jax.numpy as jnp
from jax import lax

DEVICES = 32
D = 896
FF = 4864
LAYERS = 2
NAMES = ("w_gate", "w_up", "w_down")
SHAPES = {"w_gate": (LAYERS, D, FF), "w_up": (LAYERS, D, FF), "w_down": (LAYERS, FF, D)}


def setup_inputs(seed: int = 0, part: int = 0) -> dict:
    kz, *keys = jax.random.split(jax.random.key(seed), 1 + 5 * len(NAMES))
    loud = 2.0 ** jax.random.uniform(kz, (), jnp.float32, -1.0, 1.0)
    drawn = {}
    for name, key, both in zip(NAMES, keys[:3], keys[3:6], strict=True):
        own = jax.random.normal(jax.random.fold_in(key, part), (DEVICES, *SHAPES[name]), jnp.float32)
        shared = jax.random.normal(jax.random.fold_in(both, part), SHAPES[name], jnp.float32)
        drawn["g_" + name] = (loud * (0.7 * shared / DEVICES + 0.7 * own * DEVICES**-0.5)).astype(jnp.bfloat16)
    for name, key in zip(NAMES, keys[6:9], strict=True):
        drawn[name] = (jax.random.normal(key, SHAPES[name], jnp.float32) * SHAPES[name][1] ** -0.5).astype(jnp.bfloat16)
    for name, key in zip(NAMES, keys[9:12], strict=True):
        drawn["m_" + name] = loud * 0.5 * jax.random.normal(key, SHAPES[name], jnp.float32)
    for name, key in zip(NAMES, keys[12:15], strict=True):
        drawn["v_" + name] = loud * loud * jax.random.uniform(key, SHAPES[name], jnp.float32, 0.5, 1.5)
    return drawn


def adamw(w, m, v, g):
    m = 0.9 * m + 0.1 * g
    v = 0.95 * v + 0.05 * g * g
    step = m * lax.rsqrt(v + 1e-8) + 0.1 * w
    return (w - 0.02 * step).astype(jnp.bfloat16), m, v


def reference(g_w_gate, g_w_up, g_w_down, w_gate, w_up, w_down, m_w_gate, m_w_up, m_w_down, v_w_gate, v_w_up, v_w_down):
    def total(terms):
        return lax.scan(lambda so_far, term: (so_far + term.astype(jnp.float32), None), jnp.zeros(terms.shape[1:], jnp.float32), terms)[0]

    gradients = [total(terms).astype(jnp.bfloat16).astype(jnp.float32) for terms in (g_w_gate, g_w_up, g_w_down)]
    new = [
        adamw(w.astype(jnp.float32), m, v, g)
        for w, m, v, g in zip((w_gate, w_up, w_down), (m_w_gate, m_w_up, m_w_down), (v_w_gate, v_w_up, v_w_down), gradients, strict=True)
    ]
    return tuple(one[which] for which in range(3) for one in new)
```

```python
import functools
import math

import jax
import jax.numpy as jnp
from jax import lax
from jax.experimental import pallas as pl
from jax.experimental.pallas import tpu as pltpu
from jax.sharding import PartitionSpec as P

MESH = pl.DeviceIdType.MESH
F32, BF16 = jnp.float32, jnp.bfloat16
STEP = 176
LANES, TILE = 128, 8
VMEM_MAIN = 14 * 2**20
WEIGHTS, CORES, KINDS = range(3), range(2), range(5)
DIRS = (1, -1)


def ranges(n):
    half = n // 4 // 16 * 16
    cuts = ((0, half), (half, half), (2 * half, half), (3 * half, n - 3 * half))
    return (cuts[:2], cuts[2:])


def loop(rows, body):
    full = rows // STEP
    if full == 1:
        body(0, STEP)
    elif full:
        lax.fori_loop(0, full, lambda i, _: (body(pl.multiple_of(i * STEP, 16), STEP), 0)[1], 0)
    if rows % STEP:
        body(full * STEP, rows % STEP)


def add_into(out, rows, terms, dtype=None):
    def body(at, size):
        here = pl.ds(at, size)
        total = terms[0][here, :].astype(F32)
        for term in terms[1:]:
            total += term[here, :].astype(F32)
        total = total.astype(BF16)
        out[here, :] = total if dtype is None else total.astype(dtype)

    loop(rows, body)


def moments(w, m, v, g):
    m = 0.9 * m + 0.1 * g
    v = 0.95 * v + 0.05 * g * g
    step = m * lax.rsqrt(v + 1e-8) + 0.1 * w
    return w - 0.02 * step, m, v


def kernel(side, block, forms, *refs):
    g, w, m, v, out, m_out, v_out = (refs[i : i + 3] for i in range(0, 21, 3))
    (own1, own2, grad, grad_p, w_raw, w_all, shared, mom,
     s_pair, r_pair, s_own1, s_own2, s_rs, r_p, r_q, s_in, s_grad, r_grad, s_x, r_x, s_out, s_ag, r_ag, s_fan, r_fan, free) = refs[21:]
    me = lax.axis_index("dp")
    c, y, x = me % 2, me // 2 % side, me // (2 * side)
    other = 1 - c
    pos = (x, y)
    cuts = ranges(block)
    span = [(cuts[i][0][0], cuts[i][0][1] + cuts[i][1][1]) for i in CORES]

    def at(p):
        return lax.rem(p + 2 * side, side)

    def device(axis, d):
        p = [x, y]
        p[axis] = at(pos[axis] + d)
        return {"dp": (p[0] * side + p[1]) * 2 + c}

    partner = {"dp": me + 1 - 2 * c}

    def land(k, core=None):
        return out[k].at[c if core is None else core]

    def t1(k, i, di):
        return out[k].at[other, 2, pl.ds(2 * di, 2), pl.ds(*span[i])]

    def r1(k, i, di, p):
        return out[k].at[other, di, p, pl.ds(*span[i])]

    def t2(k, i, d):
        return out[k].at[other, 3, 2, pl.ds(*cuts[i][int(d == 1)])]

    def r2(k, i, di, h):
        return out[k].at[other, 3, di, pl.ds(*cuts[i][h])]

    def remote(src, dst, send, recv, to):
        return pltpu.make_async_remote_copy(src, dst, send, recv, device_id=to, device_id_type=MESH)

    def local(src, dst, sem):
        return pltpu.make_async_copy(src, dst, sem)

    def most(k):
        return w[k].at[0, pl.ds(0, side * side - 1)]

    neighbours = [device(i, d) for i in CORES for d in DIRS]
    barrier = pltpu.get_barrier_semaphore()
    for to in (partner, *neighbours):
        pl.semaphore_signal(barrier, inc=1, device_id=to, device_id_type=MESH)
    pl.semaphore_wait(barrier, 1 + len(neighbours))

    def pair_of_blocks(ref, i, p, h):
        lo, n = span[i]
        rows = pl.ds(lo, n)
        return ref.at[p, pl.ds(2 * h, 2), rows] if i == 0 else ref.at[pl.ds(2 * h, 2), p, rows]

    def row_of_blocks(ref, i):
        lo, n = span[i]
        rows = pl.ds(lo, n)
        return ref.at[pos[0], :, rows] if i == 0 else ref.at[:, pos[1], rows]

    pieces = [(i, d) for d in DIRS for i in CORES]

    def target(s, i, d):
        hf = 1 if d == 1 else 0
        return (at(pos[i] + 2), hf) if s == 0 else (at(pos[i] + d), 1 - hf if s == 1 else hf)

    def pair_copy(k, j):
        if j < 12:
            i, d = pieces[j % 4]
            p, h = target(j // 4, i, d)
            view = functools.partial(pair_of_blocks, i=i, p=p, h=h)
        else:
            view = functools.partial(row_of_blocks, i=j - 12)
        return remote(view(g[k].at[other]), view(land(k, other)), s_pair.at[k], r_pair.at[k, j], partner)

    order1 = [(k, s, i, d) for k in WEIGHTS for s in range(3) for i, d in pieces]

    def own1_copy(n):
        k, s, i, d = order1[n]
        p, h = target(s, i, d)
        return local(pair_of_blocks(g[k].at[c], i, p, h), own1.at[n % 4, :, pl.ds(0, span[i][1])], s_own1.at[n % 4])

    def own2_copy(k, i):
        return local(row_of_blocks(g[k].at[c], i), own2.at[i, :, pl.ds(0, span[i][1])], s_own2.at[i])

    def p_copy(k, s, i, d):
        di = DIRS.index(d)
        p, h = target(s, i, d)
        dst = t1(k, i, di) if s == 0 else r1(k, i, di, pl.ds(2 * h, 2))
        return remote(pair_of_blocks(land(k), i, p, h), dst, s_rs.at[k], r_p.at[k, s, i, di], device(i, d))

    def stage_p(k, s):
        for j, (i, d) in enumerate(pieces):
            n = order1.index((k, s, i, d))
            if n + 3 < len(order1):
                own1_copy(n + 3).start()
            own1_copy(n).wait()
            pair_copy(k, s * 4 + j).wait_recv()
            if s == 2:
                p_copy(k, 0, i, d).wait_recv()
            p, h = target(s, i, d)
            sums = pair_of_blocks(land(k), i, p, h)
            for b in CORES:
                terms = [own1.at[n % 4, b], sums.at[b]]
                if s == 2:
                    terms.append(t1(k, i, DIRS.index(d)).at[b])
                add_into(sums.at[b], span[i][1], terms)
            p_copy(k, s, i, d).start()

    def q_target(s, i, d):
        hf = 1 if d == 1 else 0
        p = pos[1 - i]
        return (at(p + 2), hf) if s == 0 else (at(p + d), 1 - hf if s == 1 else hf)

    def q_rows(ref, i, p, h):
        lo, n = cuts[i][h]
        return (ref.at[pos[0], p] if i == 0 else ref.at[p, pos[1]]).at[pl.ds(lo, n)]

    def q_copy(k, s, i, d):
        di = DIRS.index(d)
        p, h = q_target(s, i, d)
        dst = t2(k, i, d) if s == 0 else r2(k, i, di, h)
        return remote(q_rows(land(k), i, p, h), dst, s_rs.at[k], r_q.at[k, s, i, di], device(1 - i, d))

    def q_terms(k, i, p, h):
        off, n = cuts[i][h][0] - span[i][0], cuts[i][h][1]
        rows = pl.ds(off, n)
        return [own2.at[i, p, rows], q_rows(land(k), i, p, h)] + [r1(k, i, di, p).at[rows] for di in CORES]

    def stage_q(k, s):
        if s == 0:
            for i in CORES:
                own2_copy(k, i).wait()
                pair_copy(k, 12 + i).wait_recv()
            for i, d in pieces:
                p_copy(k, 1, i, d).wait_recv()
                p_copy(k, 2, i, d).wait_recv()
        for i, d in pieces:
            p, h = q_target(s, i, d)
            terms = q_terms(k, i, p, h)
            if s == 2:
                q_copy(k, 0, i, d).wait_recv()
                terms.append(t2(k, i, d))
            add_into(q_rows(land(k), i, p, h), cuts[i][h][1], terms)
            q_copy(k, s, i, d).start()

    def step_loads(k):
        return [local(w[k].at[:, x * side + y], w_raw, s_in.at[0]), local(m[k], mom.at[0], s_in.at[1]), local(v[k], mom.at[1], s_in.at[2])]

    def step_stores(k):
        return [local(mom.at[0], m_out[k], s_out.at[0]), local(mom.at[1], v_out[k], s_out.at[1])]

    def own_rows(k, core):
        rows, lanes = forms[k]
        if rows % TILE == 0:
            return core * (rows * lanes), rows * lanes
        return core * (rows // TILE * TILE * lanes), (rows // TILE + 1) * TILE * lanes

    def grad_copy(k):
        lo, n = own_rows(k, other)
        rows = pl.ds(pl.multiple_of(lo, 8), n)
        return remote(grad.at[rows], grad_p.at[rows], s_grad.at[k], r_grad.at[k], partner)

    def x_copies(k):
        rows, lanes = forms[k]
        lo, n = own_rows(k, c)
        if rows % TILE == 0:
            mine = pl.ds(pl.multiple_of(lo, 8), n)
            return [remote(w_all.at[other, mine], w_all.at[other, mine], s_x.at[k, 0], r_x.at[k, 0], partner)]
        tile = TILE * lanes
        mine = pl.ds(pl.multiple_of(c * (n - 2 * tile + 2 * tile), 8), n - tile)
        middle = pl.ds(n - tile, tile)
        return [
            remote(w_all.at[other, mine], w_all.at[other, mine], s_x.at[k, 0], r_x.at[k, 0], partner),
            remote(w_all.at[other, middle], shared, s_x.at[k, 1], r_x.at[k, 1], partner),
        ]

    def take_step(k):
        rows, lanes = forms[k]

        def update(core):
            grads = (grad, grad_p) if core == 0 else (grad_p, grad)

            def one(layer, at_w, at_m):
                new_w, new_m, new_v = moments(w_all[layer, at_w, :], mom[0, at_m, :], mom[1, at_m, :], grads[layer][at_w, :])
                w_all[layer, at_w, :] = new_w
                mom[0, at_m, :] = new_m
                mom[1, at_m, :] = new_v

            if rows % TILE == 0:
                size = rows * lanes
                chunk = 8 * (rows // TILE)

                def body(n, _):
                    for layer in CORES:
                        one(layer, pl.ds(pl.multiple_of(core * size + n * chunk, 8), chunk), pl.ds(pl.multiple_of(layer * size + n * chunk, 8), chunk))
                    return 0

                lax.fori_loop(0, lanes, body, 0)
            else:
                first, last = core * rows, (core + 1) * rows
                parts = []
                r = first
                while r < last:
                    n = min(8 - r % 8, last - r)
                    parts.append((r, n))
                    r += n

                def body(lane, _):
                    for layer in CORES:
                        for r, n in parts:
                            one(layer, pl.ds((r // TILE * lanes + lane) * 8 + r % 8, n), pl.ds((r - first) * 2 * lanes + lane * 2 + layer, n, stride=2 * lanes))
                    return 0

                lax.fori_loop(0, lanes, body, 0)

        for core in CORES:
            pl.when(c == core)(functools.partial(update, core))

    def stage_step(k):
        loads = step_loads(k)
        loads[0].wait()
        for layer in CORES:

            def widen(start, size, layer=layer):
                w_all[layer, pl.ds(start, size), :] = w_raw[layer, pl.ds(start, size), :].astype(F32)

            loop(block, widen)
        for i, d in pieces:
            q_copy(k, 1, i, d).wait_recv()
            q_copy(k, 2, i, d).wait_recv()
        for i in CORES:
            for h in CORES:
                lo, n = cuts[i][h]
                terms = q_terms(k, i, pos[1 - i], h) + [r2(k, i, di, h) for di in CORES]
                add_into(grad.at[pl.ds(lo, n)], n, terms, F32)
        grad_copy(k).start()
        local(most(k), most(k), s_rs.at[k]).wait()
        for to in neighbours:
            pl.semaphore_signal(free.at[k], inc=1, device_id=to, device_id_type=MESH)
        loads[1].wait()
        loads[2].wait()
        grad_copy(k).wait_recv()
        take_step(k)
        for copy in step_stores(k):
            copy.start()
        swaps = x_copies(k)
        for copy in swaps:
            copy.start()
        for copy in swaps:
            copy.wait()
        rows, lanes = forms[k]
        if rows % TILE:
            tile = TILE * lanes
            start = rows // TILE * tile

            def merge(n, _):
                here = pl.ds(pl.multiple_of(start + n * 8, 8), 8)
                theirs = shared[pl.ds(pl.multiple_of(n * 8, 8), 8), :]
                mine = w_all[c, here, :]
                low = lax.broadcasted_iota(jnp.int32, theirs.shape, 0) < rows % TILE
                w_all[c, here, :] = jnp.where(low == (c == 0), mine, theirs)
                return 0

            lax.fori_loop(0, lanes, merge, 0)

        def narrow(start, size):
            out[k][c, x, y, pl.ds(start, size), :] = w_all[c, pl.ds(start, size), :].astype(BF16)

        loop(block, narrow)
        grad_copy(k).wait_send()
        for copy in step_stores(k):
            copy.wait()

    def place(i, first, second):
        return (second, first) if i == 0 else (first, second)

    def rows_of(i, h):
        return pl.ds(*(span[i] if h is None else cuts[i][h]))

    def ag_copy(k, i, along, d, first, second, h, event):
        dst = out[k].at[c, *place(i, first, second), rows_of(i, h)]
        return remote(dst, dst, s_ag.at[k], r_ag.at[k, i, event], device(1 - i if along == 0 else i, d))

    def fan(k, i, first, second, h):
        there = out[k].at[c, *place(i, first, second), rows_of(i, h)]
        remote(there, there, s_fan.at[k], r_fan.at[k], partner).start()

    def arrived(k, i, first, second, h, event):
        ag_copy(k, i, 0, 1, first, second, h, event).wait_recv()

    def ag_own(k):
        src = out[k].at[c, x, y]
        pl.semaphore_wait(free.at[k], len(neighbours))
        for i in CORES:
            f, s = pos[1 - i], pos[i]
            for di, d in enumerate(DIRS):
                ag_copy(k, i, 0, d, f, s, None, di).start()
            for di, d in enumerate(DIRS):
                ag_copy(k, i, 1, d, f, s, None, 4 + 5 * di).start()
        remote(src, src, s_fan.at[k], r_fan.at[k], partner).start()

    def ag_near(k):
        for di, d in enumerate(DIRS):
            for i in CORES:
                f, s = pos[1 - i], pos[i]
                from_ = at(f - d)
                arrived(k, i, from_, s, None, di)
                ag_copy(k, i, 0, d, from_, s, 1 - di, 2 + di).start()
                for d2i, d2 in enumerate(DIRS):
                    ag_copy(k, i, 1, d2, from_, s, None, 4 + 5 * d2i + 1 + di).start()
                fan(k, i, from_, s, None)

    def ag_far(k):
        for di, d in enumerate(DIRS):
            for i in CORES:
                f, s = pos[1 - i], pos[i]
                arrived(k, i, at(f + 2), s, 1 - di, 2 + di)
                for d2i, d2 in enumerate(DIRS):
                    ag_copy(k, i, 1, d2, at(f + 2), s, 1 - di, 4 + 5 * d2i + 3 + 1 - di).start()
                fan(k, i, at(f + 2), s, 1 - di)

    kinds = ((0, None, 0, 14), (-1, None, 0, 15), (1, None, 1, 16), (2, 0, 1, 17), (2, 1, 1, 18))

    def ag_second(k, which):
        for n in which:
            rel, h, onward, event = kinds[n]
            for di, d in enumerate(DIRS):
                for i in CORES:
                    f, s = pos[1 - i], pos[i]
                    first, second = at(f + rel), at(s - d)
                    arrived(k, i, first, second, h, 4 + 5 * di + n)
                    if di == onward:
                        ag_copy(k, i, 1, d, first, second, h, event).start()
                    fan(k, i, first, second, h)

    def ag_last(k):
        for n in (0, 2, 1, 3, 4):
            rel, h, _, event = kinds[n]
            for i in CORES:
                f, s = pos[1 - i], pos[i]
                arrived(k, i, at(f + rel), at(s + 2), h, event)
                fan(k, i, at(f + rel), at(s + 2), h)

    for n in range(3):
        own1_copy(n).start()
    for k in WEIGHTS:
        for j in range(14):
            pair_copy(k, j).start()

    def q12(k):
        for copy in step_loads(k):
            copy.start()
        stage_q(k, 0)
        stage_q(k, 1)

    def q3(k):
        stage_q(k, 2)

    def step(k):
        stage_step(k)
        if k < 2:
            for i in CORES:
                own2_copy(k + 1, i).start()

    for i in CORES:
        own2_copy(0, i).start()
    stage_p(0, 0), stage_p(0, 1), stage_p(0, 2), stage_p(1, 0), stage_p(1, 1)
    q12(0), stage_p(1, 2), q3(0), stage_p(2, 0), stage_p(2, 1), step(0)
    ag_own(0), q12(1), stage_p(2, 2), q3(1), ag_near(0), step(1)
    ag_own(1), q12(2), ag_far(0), q3(2), ag_second(0, (0, 1, 2)), step(2)
    ag_own(2), ag_second(0, (3, 4)), ag_near(1), ag_far(1), ag_near(2), ag_last(0), ag_second(1, KINDS), ag_far(2), ag_last(1)
    ag_second(2, KINDS), ag_last(2)

    for k in WEIGHTS:
        whole = land(k)
        local(whole, whole, s_pair.at[k]).wait()
        local(most(k), most(k), s_ag.at[k]).wait()
        local(whole, whole, s_fan.at[k]).wait()
        local(whole, whole, r_fan.at[k]).wait()


def spread(*refs):
    n = (len(refs) - 3) // 2
    buffer, s_in, s_out = refs[2 * n :]
    lanes = buffer.shape[2]
    for a in range(n):

        def load(lane, _, a=a):
            columns = pl.ds(pl.multiple_of(lane * LANES, LANES), LANES)
            pltpu.make_async_copy(refs[a].at[:, :, columns], buffer.at[a, :, lane], s_in.at[a]).start()
            return 0

        lax.fori_loop(0, lanes, load, 0)
    for a in range(n):
        pltpu.make_async_copy(refs[n + a], buffer.at[a], s_in.at[a]).wait()
        pltpu.make_async_copy(buffer.at[a], refs[n + a], s_out.at[a]).start()
    for a in range(n):
        pltpu.make_async_copy(buffer.at[a], refs[n + a], s_out.at[a]).wait()


def deliver(*refs):
    n = (len(refs) - 4) // 2
    src, dst, (buffer, s_w, s_in, s_out) = refs[:n], refs[n : 2 * n], refs[2 * n :]
    big = len(WEIGHTS)

    def load(j):
        return pltpu.make_async_copy(src[big + j], buffer.at[j], s_in.at[j])

    def store(j):
        return pltpu.make_async_copy(buffer.at[j], dst[big + j], s_out.at[j])

    for j in range(n - big):
        load(j).start()
    for k in WEIGHTS:
        for core in CORES:
            for x in range(src[k].shape[1]):
                pltpu.make_async_copy(src[k].at[core, x], dst[k].at[core, x], s_w.at[k]).start()
    for j in range(n - big):
        load(j).wait()
        store(j).start()
    for j in range(n - big):
        store(j).wait()
    for k in WEIGHTS:
        pltpu.make_async_copy(src[k], dst[k], s_w.at[k]).wait()


def tiles(a, chips):
    layers, rows, columns = a.shape
    a = a.reshape(layers, rows // TILE, TILE, columns // LANES, LANES).transpose(0, 1, 3, 2, 4)
    return a.reshape(layers, chips, -1, LANES)


def untiles(a, shape):
    layers, rows, columns = shape
    a = a.reshape(layers, rows // TILE, columns // LANES, TILE, LANES).transpose(0, 1, 3, 2, 4)
    return a.reshape(shape)


def moment_rows(arrays):
    odd = [a.transpose(1, 0, 2) for a in arrays if a.shape[1] % TILE]
    shapes = [(a.shape[0], a.shape[2] // LANES, a.shape[1], LANES) for a in odd]
    dma = pltpu.SemaphoreType.DMA((len(odd),))
    done = iter(
        pl.pallas_call(
            spread,
            out_shape=[jax.ShapeDtypeStruct(shape, F32) for shape in shapes],
            in_specs=[pl.BlockSpec(memory_space=pl.ANY)] * len(odd),
            out_specs=[pl.BlockSpec(memory_space=pl.ANY)] * len(odd),
            scratch_shapes=[pltpu.VMEM((len(odd), *shapes[0]), F32), dma, dma],
        )(*odd)
    )
    return [next(done).reshape(-1, LANES) if a.shape[1] % TILE else tiles(a, 1).reshape(-1, LANES) for a in arrays]


def moment_back(a, shape):
    layers, rows, columns = shape
    if rows % TILE == 0:
        return untiles(a, shape)
    return a.reshape(rows, columns // LANES, layers, 128).transpose(0, 2, 1, 3).reshape(rows, layers, columns).transpose(1, 0, 2)


def solution(mesh):
    n = mesh.shape["dp"]
    side = math.isqrt(n // 2)
    chips = side * side
    assert 2 * chips == n and side == 4

    def step(*arrays):
        terms, weights, m, v = (arrays[i : i + 3] for i in (0, 3, 6, 9))
        shapes, m_shapes = [a.shape for a in weights], [a.shape for a in m]
        block = math.prod(shapes[0][1:]) // chips // LANES
        forms = [(s[1], s[2] // LANES) for s in m_shapes]
        cuts = ranges(block)
        wide = max(sum(h[1] for h in i) for i in cuts)
        odd = max([lanes * TILE for rows, lanes in forms if rows % TILE] + [8])
        split = (2, side, side, block, LANES)
        operands = (
            [tiles(t[0], chips).reshape(split) for t in terms] + [tiles(a, chips) for a in weights] + moment_rows(m + v)
        )
        dma = pltpu.SemaphoreType.DMA
        moment = jax.ShapeDtypeStruct(operands[6].shape, F32)
        anywhere = pl.BlockSpec(memory_space=pl.ANY)
        made = pl.pallas_call(
            functools.partial(kernel, side, block, forms),
            out_shape=[pltpu.VMEM(split, BF16)] * 3 + [moment] * 6,
            in_specs=[anywhere] * 12,
            out_specs=[pl.BlockSpec(memory_space=pltpu.VMEM)] * 3 + [anywhere] * 6,
            scratch_shapes=[
                pltpu.VMEM((4, 2, wide, LANES), BF16),
                pltpu.VMEM((2, side, wide, LANES), BF16),
                pltpu.VMEM((block, LANES), F32),
                pltpu.VMEM((block, LANES), F32),
                pltpu.VMEM((2, block, LANES), BF16),
                pltpu.VMEM((2, block, LANES), F32),
                pltpu.VMEM((odd, LANES), F32),
                pltpu.VMEM((2, *moment.shape), F32),
                *(dma(shape) for shape in ((3,), (3, 14), (4,), (2,), (3,), (3, 3, 2, 2), (3, 3, 2, 2), (3,), (3,), (3,), (3, 2), (3, 2), (2,), (3,), (3, 2, 19), (3,), (3,))),
                pltpu.SemaphoreType.REGULAR((3,)),
            ],
            compiler_params=pltpu.CompilerParams(collective_id=0, has_side_effects=True, vmem_limit_bytes=VMEM_MAIN),
        )(*operands)
        made = [*(pltpu.with_memory_space_constraint(a, pltpu.VMEM) for a in made[:3]), *made[3:]]
        results = pl.pallas_call(
            deliver,
            out_shape=[jax.ShapeDtypeStruct(a.shape, a.dtype) for a in made],
            in_specs=[anywhere] * 9,
            out_specs=[anywhere] * 9,
            scratch_shapes=[pltpu.VMEM((6, *moment.shape), F32), dma((3,)), dma((6,)), dma((6,))],
            compiler_params=pltpu.CompilerParams(vmem_limit_bytes=VMEM_MAIN),
        )(*made)
        new = [untiles(a, s) for a, s in zip(results[:3], shapes, strict=True)]
        return (*new, *(moment_back(a, s) for a, s in zip(results[3:], m_shapes * 2, strict=True)))

    all_of, cut = P(None, None, None), P(None, "dp", None)
    return jax.shard_map(
        step,
        mesh=mesh,
        in_specs=(P(("rep", "dp"), None, None, None),) * 3 + (all_of,) * 3 + (cut,) * 6,
        out_specs=(P("rep", None, None),) * 3 + (P("rep", "dp", None),) * 6,
        check_vma=False,
    )
```

```python
import functools
import math

import jax
import jax.numpy as jnp
from jax import lax
from jax.experimental import pallas as pl
from jax.experimental.layout import Layout, with_layout_constraint
from jax.experimental.pallas import tpu as pltpu
from jax.sharding import PartitionSpec as P

MESH = pl.DeviceIdType.MESH
F32, BF16 = jnp.float32, jnp.bfloat16
STEP, SLOTS = 176, 4
LANES, TILE = 128, 8
VMEM_MAIN = 10116 * 2**10
IN_HBM = 1
WEIGHTS, CORES = range(3), range(2)
DIRS = (1, -1)
SCHEDULE = (
    "P00 P01 P02 P10",
    "P11 Q00 Q01 P12",
    "Q02 P20 P21 F0",
    "Q10 Q11 O0 P22",
    "Q12 N0 F1 Q20",
    "S02 X0 Q21 Q22",
    "O1 N1 S01 F2",
    "S00 O2 S03 S04",
    "L02 X1 L01 S10",
    "N2 L04 L00 S14",
    "L03 S11 S12 S13",
    "X2 S20 L10 L14",
    "L13 L12 L11 S21",
    "S22 S23 S24 L21",
    "L20 L22 L23 L24",
)


def ranges(n, k):
    half = n // 4 // 16 * 16
    rows = [half] * 4
    rows[1 + 2 * ((k + 1) % 2)] += n - 4 * half
    cuts = [(sum(rows[:j]), rows[j]) for j in range(4)]
    return (cuts[:2], cuts[2:])


def loop(rows, body):
    full = rows // STEP
    if full == 1:
        body(0, STEP)
    elif full:
        lax.fori_loop(0, full, lambda i, _: (body(pl.multiple_of(i * STEP, 16), STEP), 0)[1], 0)
    if rows % STEP:
        body(full * STEP, rows % STEP)


def add_into(out, rows, terms, dtype=None):
    def body(at, size):
        here = pl.ds(at, size)
        total = terms[0][here, :].astype(F32)
        for term in terms[1:]:
            total += term[here, :].astype(F32)
        total = total.astype(BF16)
        out[here, :] = total if dtype is None else total.astype(dtype)

    loop(rows, body)


def moments(w, m, v, g):
    m = 0.9 * m + 0.1 * g
    v = 0.95 * v + 0.05 * g * g
    step = m * lax.rsqrt(v + 1e-8) + 0.1 * w
    return w - 0.02 * step, m, v


def kernel(side, block, forms, *refs):
    g, w, m, v, out, m_out, v_out = (refs[i : i + 3] for i in range(0, 21, 3))
    (own1, own2, grad, grad_p, w_raw, w_all, shared,
     s_pair, r_pair, s_own1, s_own2, s_rs, r_p, r_q, s_in, s_grad, r_grad, s_x, r_x, s_out, s_ag, r_ag, s_fan, r_fan, r_first, free) = refs[21:]
    me = lax.axis_index("dp")
    c, y, x = me % 2, me // 2 % side, me // (2 * side)
    other = 1 - c
    pos = (x, y)
    cuts = [ranges(block, k) for k in WEIGHTS]
    span = [[(i[0][0], i[0][1] + i[1][1]) for i in cuts[k]] for k in WEIGHTS]

    def at(p):
        return lax.rem(p + 2 * side, side)

    def device(axis, d):
        p = [x, y]
        p[axis] = at(pos[axis] + d)
        return {"dp": (p[0] * side + p[1]) * 2 + c}

    partner = {"dp": me + 1 - 2 * c}

    def land(k, core=None):
        return out[k].at[c if core is None else core]

    def t1(k, i, di):
        return out[k].at[other, 2, pl.ds(2 * di, 2), pl.ds(*span[k][i])]

    def r1(k, i, di, p):
        return out[k].at[other, di, p, pl.ds(*span[k][i])]

    def t2(k, i, d):
        return out[k].at[other, 3, 2, pl.ds(*cuts[k][i][int(d == 1)])]

    def r2(k, i, di, h):
        return out[k].at[other, 3, di, pl.ds(*cuts[k][i][h])]

    def remote(src, dst, send, recv, to):
        return pltpu.make_async_remote_copy(src, dst, send, recv, device_id=to, device_id_type=MESH)

    def local(src, dst, sem):
        return pltpu.make_async_copy(src, dst, sem)

    def most(k):
        return w[k].at[0, pl.ds(0, side * side - 1)]

    def pair_of_blocks(ref, k, i, p, h):
        lo, n = span[k][i]
        rows = pl.ds(lo, n)
        return ref.at[p, pl.ds(2 * h, 2), rows] if i == 0 else ref.at[pl.ds(2 * h, 2), p, rows]

    def row_of_blocks(ref, k, i):
        lo, n = span[k][i]
        rows = pl.ds(lo, n)
        return ref.at[pos[0], :, rows] if i == 0 else ref.at[:, pos[1], rows]

    pieces = [(i, d) for d in DIRS for i in CORES]

    def target(s, i, d):
        hf = 1 if d == 1 else 0
        return (at(pos[i] + 2), hf) if s == 0 else (at(pos[i] + d), 1 - hf if s == 1 else hf)

    def pair_copy(k, j):
        if j < 12:
            i, d = pieces[j % 4]
            p, h = target(j // 4, i, d)
            view = functools.partial(pair_of_blocks, k=k, i=i, p=p, h=h)
        else:
            view = functools.partial(row_of_blocks, k=k, i=j - 12)
        return remote(view(g[k].at[other]), view(land(k, other)), s_pair.at[k], r_pair.at[k, j], partner)

    quarters = [(b, h) for b in CORES for h in CORES]

    def quarter(ref, i, d, b, h):
        p, half = target(0, i, d)
        rows = pl.ds(*cuts[0][i][h])
        return ref.at[p, 2 * half + b, rows] if i == 0 else ref.at[2 * half + b, p, rows]

    def first_pair(i, d, b, h):
        return remote(quarter(g[0].at[other], i, d, b, h), quarter(land(0, other), i, d, b, h), s_pair.at[0], r_first.at[0, i, DIRS.index(d), b, h], partner)

    def first_send(i, d, b, h):
        lo, n = cuts[0][i][h]
        dst = t1(0, i, DIRS.index(d)).at[b, pl.ds(lo - span[0][i][0], n)]
        return remote(quarter(land(0), i, d, b, h), dst, s_rs.at[0], r_first.at[1, i, DIRS.index(d), b, h], device(i, d))

    def stage_first():
        for b, h in quarters:
            for j, (i, d) in enumerate(pieces):
                if (b, h) == quarters[0]:
                    own1_copy(j).wait()
                first_pair(i, d, b, h).wait_recv()
                lo, n = cuts[0][i][h]
                sums = quarter(land(0), i, d, b, h)
                add_into(sums, n, [own1.at[j % SLOTS, b, pl.ds(lo - span[0][i][0], n)], sums])
                first_send(i, d, b, h).start()
        for n in range(SLOTS, 2 * SLOTS - 1):
            own1_copy(n).start()

    order1 = [(k, s, i, d) for k in WEIGHTS for s in range(3) for i, d in pieces]

    def own1_copy(n):
        k, s, i, d = order1[n]
        p, h = target(s, i, d)
        return local(pair_of_blocks(g[k].at[c], k, i, p, h), own1.at[n % SLOTS, :, pl.ds(0, span[k][i][1])], s_own1.at[n % SLOTS])

    def own2_copy(k, i):
        return local(row_of_blocks(g[k].at[c], k, i), own2.at[i, :, pl.ds(0, span[k][i][1])], s_own2.at[i])

    def p_copy(k, s, i, d):
        di = DIRS.index(d)
        p, h = target(s, i, d)
        dst = t1(k, i, di) if s == 0 else r1(k, i, di, pl.ds(2 * h, 2))
        return remote(pair_of_blocks(land(k), k, i, p, h), dst, s_rs.at[k], r_p.at[k, s, i, di], device(i, d))

    def stage_p(k, s):
        if k + s == 0:
            return stage_first()
        for j, (i, d) in enumerate(pieces):
            n = order1.index((k, s, i, d))
            if n + SLOTS - 1 < len(order1):
                own1_copy(n + SLOTS - 1).start()
            own1_copy(n).wait()
            pair_copy(k, s * 4 + j).wait_recv()
            if s == 2 and k == 0:
                for b, h in quarters:
                    first_send(i, d, b, h).wait_recv()
            elif s == 2:
                p_copy(k, 0, i, d).wait_recv()
            p, h = target(s, i, d)
            sums = pair_of_blocks(land(k), k, i, p, h)
            for b in CORES:
                terms = [own1.at[n % SLOTS, b], sums.at[b]]
                if s == 2:
                    terms.append(t1(k, i, DIRS.index(d)).at[b])
                add_into(sums.at[b], span[k][i][1], terms)
            p_copy(k, s, i, d).start()

    def q_target(s, i, d):
        hf = 1 if d == 1 else 0
        p = pos[1 - i]
        return (at(p + 2), hf) if s == 0 else (at(p + d), 1 - hf if s == 1 else hf)

    def q_rows(ref, k, i, p, h):
        lo, n = cuts[k][i][h]
        return (ref.at[pos[0], p] if i == 0 else ref.at[p, pos[1]]).at[pl.ds(lo, n)]

    def q_copy(k, s, i, d):
        di = DIRS.index(d)
        p, h = q_target(s, i, d)
        dst = t2(k, i, d) if s == 0 else r2(k, i, di, h)
        return remote(q_rows(land(k), k, i, p, h), dst, s_rs.at[k], r_q.at[k, s, i, di], device(1 - i, d))

    def q_terms(k, i, p, h):
        off, n = cuts[k][i][h][0] - span[k][i][0], cuts[k][i][h][1]
        rows = pl.ds(off, n)
        return [own2.at[i, p, rows], q_rows(land(k), k, i, p, h)] + [r1(k, i, di, p).at[rows] for di in CORES]

    def stage_q(k, s):
        if s == 0:
            for i in CORES:
                own2_copy(k, i).wait()
                pair_copy(k, 12 + i).wait_recv()
            for i, d in pieces:
                p_copy(k, 1, i, d).wait_recv()
                p_copy(k, 2, i, d).wait_recv()
        for i, d in pieces:
            p, h = q_target(s, i, d)
            terms = q_terms(k, i, p, h)
            if s == 2:
                q_copy(k, 0, i, d).wait_recv()
                terms.append(t2(k, i, d))
            add_into(q_rows(land(k), k, i, p, h), cuts[k][i][h][1], terms)
            q_copy(k, s, i, d).start()

    def moment_refs(k):
        return m_out[max(k, IN_HBM)], v_out[max(k, IN_HBM)]

    def step_loads(k):
        new_m, new_v = moment_refs(k)
        return [local(w[k].at[:, x * side + y], w_raw, s_in.at[0]), local(m[k], new_m, s_in.at[1]), local(v[k], new_v, s_in.at[2])]

    def step_stores(k):
        if k >= IN_HBM:
            return []
        new_m, new_v = moment_refs(k)
        return [local(new_m, m_out[k], s_out.at[0]), local(new_v, v_out[k], s_out.at[1])]

    def own_rows(k, core):
        rows, lanes = forms[k]
        if rows % TILE == 0:
            return core * (rows * lanes), rows * lanes
        return core * (rows // TILE * TILE * lanes), (rows // TILE + 1) * TILE * lanes

    def grad_copy(k):
        lo, n = own_rows(k, other)
        rows = pl.ds(pl.multiple_of(lo, 8), n)
        return remote(grad.at[rows], grad_p.at[rows], s_grad.at[k], r_grad.at[k], partner)

    def x_copies(k):
        rows, lanes = forms[k]
        lo, n = own_rows(k, c)
        if rows % TILE == 0:
            mine = pl.ds(pl.multiple_of(lo, 8), n)
            return [remote(w_all.at[other, mine], w_all.at[other, mine], s_x.at[k, 0], r_x.at[k, 0], partner)]
        tile = TILE * lanes
        mine = pl.ds(pl.multiple_of(c * (n - 2 * tile + 2 * tile), 8), n - tile)
        middle = pl.ds(n - tile, tile)
        return [
            remote(w_all.at[other, mine], w_all.at[other, mine], s_x.at[k, 0], r_x.at[k, 0], partner),
            remote(w_all.at[other, middle], shared, s_x.at[k, 1], r_x.at[k, 1], partner),
        ]

    def take_step(k):
        rows, lanes = forms[k]

        def update(core):
            grads = (grad, grad_p) if core == 0 else (grad_p, grad)
            m_ref, v_ref = moment_refs(k)

            def one(layer, at_w, at_m):
                new_w, new_m, new_v = moments(w_all[layer, at_w, :], m_ref[at_m, :], v_ref[at_m, :], grads[layer][at_w, :])
                w_all[layer, at_w, :] = new_w
                m_ref[at_m, :] = new_m
                v_ref[at_m, :] = new_v

            if rows % TILE == 0:
                size = rows * lanes
                chunk = 8 * (rows // TILE)

                def body(n, _):
                    for layer in CORES:
                        one(layer, pl.ds(pl.multiple_of(core * size + n * chunk, 8), chunk), pl.ds(pl.multiple_of(layer * size + n * chunk, 8), chunk))
                    return 0

                lax.fori_loop(0, lanes, body, 0)
            else:
                first, last = core * rows, (core + 1) * rows
                parts = []
                r = first
                while r < last:
                    n = min(8 - r % 8, last - r)
                    parts.append((r, n))
                    r += n

                def body(lane, _):
                    for layer in CORES:
                        for r, n in parts:
                            one(layer, pl.ds((r // TILE * lanes + lane) * 8 + r % 8, n), pl.ds((r - first) * 2 * lanes + lane * 2 + layer, n, stride=2 * lanes))
                    return 0

                lax.fori_loop(0, lanes, body, 0)

        for core in CORES:
            pl.when(c == core)(functools.partial(update, core))

    def stage_step(k):
        loads = step_loads(k)
        loads[0].wait()
        for layer in CORES:

            def widen(start, size, layer=layer):
                w_all[layer, pl.ds(start, size), :] = w_raw[layer, pl.ds(start, size), :].astype(F32)

            loop(block, widen)
        for i, d in pieces:
            q_copy(k, 1, i, d).wait_recv()
            q_copy(k, 2, i, d).wait_recv()
        for i in CORES:
            for h in CORES:
                lo, n = cuts[k][i][h]
                terms = q_terms(k, i, pos[1 - i], h) + [r2(k, i, di, h) for di in CORES]
                add_into(grad.at[pl.ds(lo, n)], n, terms, F32)
        grad_copy(k).start()
        local(most(k), most(k), s_rs.at[k]).wait()
        for to in neighbours:
            pl.semaphore_signal(free.at[k], inc=1, device_id=to, device_id_type=MESH)
        loads[1].wait()
        loads[2].wait()
        grad_copy(k).wait_recv()
        take_step(k)
        for copy in step_stores(k):
            copy.start()
        swaps = x_copies(k)
        for copy in swaps:
            copy.start()
        for copy in swaps:
            copy.wait()
        rows, lanes = forms[k]
        if rows % TILE:
            tile = TILE * lanes
            start = rows // TILE * tile

            def merge(n, _):
                here = pl.ds(pl.multiple_of(start + n * 8, 8), 8)
                theirs = shared[pl.ds(pl.multiple_of(n * 8, 8), 8), :]
                mine = w_all[c, here, :]
                low = lax.broadcasted_iota(jnp.int32, theirs.shape, 0) < rows % TILE
                w_all[c, here, :] = jnp.where(low == (c == 0), mine, theirs)
                return 0

            lax.fori_loop(0, lanes, merge, 0)

        def narrow(start, size):
            out[k][c, x, y, pl.ds(start, size), :] = w_all[c, pl.ds(start, size), :].astype(BF16)

        loop(block, narrow)
        grad_copy(k).wait_send()
        for copy in step_stores(k):
            copy.wait()

    def place(i, first, second):
        return (second, first) if i == 0 else (first, second)

    def rows_of(k, i, h):
        return pl.ds(*(span[k][i] if h is None else cuts[k][i][h]))

    def ag_copy(k, i, along, d, first, second, h, event):
        dst = out[k].at[c, *place(i, first, second), rows_of(k, i, h)]
        return remote(dst, dst, s_ag.at[k], r_ag.at[k, i, event], device(1 - i if along == 0 else i, d))

    def fan(k, i, first, second, h):
        there = out[k].at[c, *place(i, first, second), rows_of(k, i, h)]
        remote(there, there, s_fan.at[k], r_fan.at[k], partner).start()

    def arrived(k, i, first, second, h, event):
        ag_copy(k, i, 0, 1, first, second, h, event).wait_recv()

    def ag_own(k):
        src = out[k].at[c, x, y]
        pl.semaphore_wait(free.at[k], len(neighbours))
        for i in CORES:
            f, s = pos[1 - i], pos[i]
            for di, d in enumerate(DIRS):
                ag_copy(k, i, 0, d, f, s, None, di).start()
            for di, d in enumerate(DIRS):
                ag_copy(k, i, 1, d, f, s, None, 4 + 5 * di).start()
        remote(src, src, s_fan.at[k], r_fan.at[k], partner).start()

    def ag_near(k):
        for di, d in enumerate(DIRS):
            for i in CORES:
                f, s = pos[1 - i], pos[i]
                from_ = at(f - d)
                arrived(k, i, from_, s, None, di)
                ag_copy(k, i, 0, d, from_, s, 1 - di, 2 + di).start()
                for d2i, d2 in enumerate(DIRS):
                    ag_copy(k, i, 1, d2, from_, s, None, 4 + 5 * d2i + 1 + di).start()
                fan(k, i, from_, s, None)

    def ag_far(k):
        for di, d in enumerate(DIRS):
            for i in CORES:
                f, s = pos[1 - i], pos[i]
                arrived(k, i, at(f + 2), s, 1 - di, 2 + di)
                for d2i, d2 in enumerate(DIRS):
                    ag_copy(k, i, 1, d2, at(f + 2), s, 1 - di, 4 + 5 * d2i + 3 + 1 - di).start()
                fan(k, i, at(f + 2), s, 1 - di)

    kinds = ((0, None, 0, 14), (-1, None, 0, 15), (1, None, 1, 16), (2, 0, 1, 17), (2, 1, 1, 18))

    def ag_second(k, n):
        rel, h, onward, event = kinds[n]
        for di, d in enumerate(DIRS):
            for i in CORES:
                f, s = pos[1 - i], pos[i]
                first, second = at(f + rel), at(s - d)
                arrived(k, i, first, second, h, 4 + 5 * di + n)
                if di == onward:
                    ag_copy(k, i, 1, d, first, second, h, event).start()
                fan(k, i, first, second, h)

    def ag_last(k, n):
        rel, h, _, event = kinds[n]
        for i in CORES:
            f, s = pos[1 - i], pos[i]
            arrived(k, i, at(f + rel), at(s + 2), h, event)
            fan(k, i, at(f + rel), at(s + 2), h)

    neighbours = [device(i, d) for i in CORES for d in DIRS]
    barrier = pltpu.get_barrier_semaphore()
    for to in (partner, *neighbours):
        pl.semaphore_signal(barrier, inc=1, device_id=to, device_id_type=MESH)
    for n in range(SLOTS):
        own1_copy(n).start()
    for i in CORES:
        own2_copy(0, i).start()
    pl.semaphore_wait(barrier, 1 + len(neighbours))
    for b, h in quarters:
        for i, d in pieces:
            first_pair(i, d, b, h).start()
    for k in WEIGHTS:
        for j in range(0 if k else len(pieces), 14):
            pair_copy(k, j).start()

    def stage_q_with_loads(k, s):
        if s == 0:
            for copy in step_loads(k):
                copy.start()
        stage_q(k, s)

    def stage_f(k):
        stage_step(k)
        if k + 1 < len(WEIGHTS):
            for i in CORES:
                own2_copy(k + 1, i).start()

    tasks = {"P": stage_p, "Q": stage_q_with_loads, "F": stage_f, "O": ag_own, "N": ag_near, "X": ag_far, "S": ag_second, "L": ag_last}
    for line in SCHEDULE:
        for task in line.split():
            tasks[task[0]](*(int(digit) for digit in task[1:]))

    for k in WEIGHTS:
        whole = land(k)
        local(whole, whole, s_pair.at[k]).wait()
        local(most(k), most(k), s_ag.at[k]).wait()
        local(whole, whole, s_fan.at[k]).wait()
        local(whole, whole, r_fan.at[k]).wait()


def deliver(*refs):
    n = (len(refs) - 4) // 2
    src, dst, (buffer, s_in, s_out, s_pass) = refs[:n], refs[n : 2 * n], refs[2 * n :]
    through = [j for j in range(len(WEIGHTS), n) if j % len(WEIGHTS) < IN_HBM]
    copies = []
    for at, j in enumerate(through):
        pltpu.make_async_copy(src[j], buffer.at[at], s_in.at[at]).start()
    for j in range(n):
        if j in through:
            continue
        if j < len(WEIGHTS):
            for core in CORES:
                for x in range(src[j].shape[1]):
                    pltpu.make_async_copy(src[j].at[core, x], dst[j].at[core, x], s_out.at[j]).start()
        else:
            pltpu.make_async_copy(src[j], dst[j], s_out.at[j]).start()
        copies.append(pltpu.make_async_copy(src[j], dst[j], s_out.at[j]))
    for at, j in enumerate(through):
        pltpu.make_async_copy(src[j], buffer.at[at], s_in.at[at]).wait()
        copies.append(pltpu.make_async_copy(buffer.at[at], dst[j], s_pass.at[at]))
        copies[-1].start()
    for copy in copies:
        copy.wait()


def tiles(a, chips):
    layers, rows, columns = a.shape
    a = a.reshape(layers, rows // TILE, TILE, columns // LANES, LANES).transpose(0, 1, 3, 2, 4)
    return a.reshape(layers, chips, -1, LANES)


def untiles(a, shape):
    layers, rows, columns = shape
    a = a.reshape(layers, rows // TILE, columns // LANES, TILE, LANES).transpose(0, 1, 3, 2, 4)
    return a.reshape(shape)


def moment_rows(a):
    layers, rows, columns = a.shape
    if rows % TILE == 0:
        return tiles(a, 1).reshape(-1, LANES)
    a = with_layout_constraint(a.reshape(layers, rows, columns // LANES, LANES), Layout(major_to_minor=(1, 2, 0, 3)))
    return a.transpose(1, 2, 0, 3).reshape(-1, LANES)


def moment_back(a, shape):
    layers, rows, columns = shape
    if rows % TILE == 0:
        return untiles(a, shape)
    return a.reshape(rows, columns // LANES, layers, 128).transpose(0, 2, 1, 3).reshape(rows, layers, columns).transpose(1, 0, 2)


def solution(mesh):
    n = mesh.shape["dp"]
    side = math.isqrt(n // 2)
    chips = side * side
    assert 2 * chips == n and side == 4

    def step(*arrays):
        terms, weights, m, v = (arrays[i : i + 3] for i in (0, 3, 6, 9))
        shapes, m_shapes = [a.shape for a in weights], [a.shape for a in m]
        block = math.prod(shapes[0][1:]) // chips // LANES
        forms = [(s[1], s[2] // LANES) for s in m_shapes]
        wide = max(sum(h[1] for h in i) for i in ranges(block, 0))
        odd = max([lanes * TILE for rows, lanes in forms if rows % TILE] + [8])
        split = (2, side, side, block, LANES)
        operands = (
            [tiles(t[0], chips).reshape(split) for t in terms] + [tiles(a, chips) for a in weights] + [moment_rows(a) for a in m + v]
        )
        dma = pltpu.SemaphoreType.DMA
        moment = jax.ShapeDtypeStruct(operands[6].shape, F32)
        anywhere, vmem = pl.BlockSpec(memory_space=pl.ANY), pl.BlockSpec(memory_space=pltpu.VMEM)
        made = pl.pallas_call(
            functools.partial(kernel, side, block, forms),
            out_shape=[pltpu.VMEM(split, BF16)] * 3 + ([moment] * IN_HBM + [pltpu.VMEM(moment.shape, F32)] * (3 - IN_HBM)) * 2,
            in_specs=[anywhere] * 12,
            out_specs=[vmem] * 3 + ([anywhere] * IN_HBM + [vmem] * (3 - IN_HBM)) * 2,
            scratch_shapes=[
                pltpu.VMEM((SLOTS, 2, wide, LANES), BF16),
                pltpu.VMEM((2, side, wide, LANES), BF16),
                pltpu.VMEM((block, LANES), F32),
                pltpu.VMEM((block, LANES), F32),
                pltpu.VMEM((2, block, LANES), BF16),
                pltpu.VMEM((2, block, LANES), F32),
                pltpu.VMEM((odd, LANES), F32),
                *(dma(shape) for shape in ((3,), (3, 14), (SLOTS,), (2,), (3,), (3, 3, 2, 2), (3, 3, 2, 2), (3,), (3,), (3,), (3, 2), (3, 2), (2,), (3,), (3, 2, 19), (3,), (3,), (2,) * 5)),
                pltpu.SemaphoreType.REGULAR((3,)),
            ],
            compiler_params=pltpu.CompilerParams(collective_id=0, has_side_effects=True, vmem_limit_bytes=VMEM_MAIN),
        )(*operands)
        made = [a if j >= 3 and j % 3 < IN_HBM else pltpu.with_memory_space_constraint(a, pltpu.VMEM) for j, a in enumerate(made)]
        results = pl.pallas_call(
            deliver,
            out_shape=[jax.ShapeDtypeStruct(a.shape, a.dtype) for a in made],
            in_specs=[anywhere] * 9,
            out_specs=[anywhere] * 9,
            scratch_shapes=[pltpu.VMEM((2 * IN_HBM, *moment.shape), F32), dma((2 * IN_HBM,)), dma((len(made),)), dma((2 * IN_HBM,))],
            compiler_params=pltpu.CompilerParams(vmem_limit_bytes=VMEM_MAIN),
        )(*made)
        new = [untiles(a, s) for a, s in zip(results[:3], shapes, strict=True)]
        return (*new, *(moment_back(a, s) for a, s in zip(results[3:], m_shapes * 2, strict=True)))

    all_of, cut = P(None, None, None), P(None, "dp", None)
    return jax.shard_map(
        step,
        mesh=mesh,
        in_specs=(P(("rep", "dp"), None, None, None),) * 3 + (all_of,) * 3 + (cut,) * 6,
        out_specs=(P("rep", None, None),) * 3 + (P("rep", "dp", None),) * 6,
        check_vma=False,
    )
```

```python
import functools
import math

import jax
import jax.numpy as jnp
from jax import lax
from jax.experimental import pallas as pl
from jax.experimental.layout import Layout, with_layout_constraint
from jax.experimental.pallas import tpu as pltpu
from jax.sharding import PartitionSpec as P

MESH = pl.DeviceIdType.MESH
F32, BF16 = jnp.float32, jnp.bfloat16
STEP, SLOTS = 176, 4
LANES, TILE = 128, 8
VMEM_MAIN = 10116 * 2**10
IN_HBM = 1
WEIGHTS, CORES = range(3), range(2)
DIRS = (1, -1)
SCHEDULE = (
    "P00 P01 P02 P10",
    "P11 Q00 Q01 P12",
    "Q02 P20 P21 F0",
    "O0 Q10 Q11 P22",
    "Q12 N0 F1 O1",
    "Q20 Q21 X0 Q22",
    "S00 S01 S02 S03",
    "S04 F2 O2 N1",
    "X1 N2 L00 L02",
    "L01 L03 L04 S10",
    "S11 S12 S13 S14",
    "X2 L10 L12 L11",
    "L13 L14 S20 S21",
    "S22 S23 S24 L20",
    "L22 L21 L23 L24",
)


def ranges(n, k):
    half = n // 4 // 16 * 16
    rows = [half] * 4
    rows[1 + 2 * ((k + 1) % 2)] += n - 4 * half
    cuts = [(sum(rows[:j]), rows[j]) for j in range(4)]
    return (cuts[:2], cuts[2:])


def loop(rows, body):
    full = rows // STEP
    if full == 1:
        body(0, STEP)
    elif full:
        lax.fori_loop(0, full, lambda i, _: (body(pl.multiple_of(i * STEP, 16), STEP), 0)[1], 0)
    if rows % STEP:
        body(full * STEP, rows % STEP)


def add_into(out, rows, terms, dtype=None):
    def body(at, size):
        here = pl.ds(at, size)
        total = terms[0][here, :].astype(F32)
        for term in terms[1:]:
            total += term[here, :].astype(F32)
        total = total.astype(BF16)
        out[here, :] = total if dtype is None else total.astype(dtype)

    loop(rows, body)


def moments(w, m, v, g):
    m = 0.9 * m + 0.1 * g
    v = 0.95 * v + 0.05 * g * g
    step = m * lax.rsqrt(v + 1e-8) + 0.1 * w
    return w - 0.02 * step, m, v


def kernel(side, block, forms, *refs):
    g, w, m, v, out, m_out, v_out = (refs[i : i + 3] for i in range(0, 21, 3))
    (own1, own2, grad, grad_p, w_raw, w_all, shared,
     s_pair, r_pair, s_own1, s_own2, s_rs, r_p, r_q, s_in, s_grad, r_grad, s_x, r_x, s_out, s_ag, r_ag, s_fan, r_fan, r_first, free) = refs[21:]
    me = lax.axis_index("dp")
    c, y, x = me % 2, me // 2 % side, me // (2 * side)
    other = 1 - c
    pos = (x, y)
    cuts = [ranges(block, k) for k in WEIGHTS]
    span = [[(i[0][0], i[0][1] + i[1][1]) for i in cuts[k]] for k in WEIGHTS]

    def at(p):
        return lax.rem(p + 2 * side, side)

    def device(axis, d):
        p = [x, y]
        p[axis] = at(pos[axis] + d)
        return {"dp": (p[0] * side + p[1]) * 2 + c}

    partner = {"dp": me + 1 - 2 * c}

    def land(k, core=None):
        return out[k].at[c if core is None else core]

    def t1(k, i, di):
        return out[k].at[other, 2, pl.ds(2 * di, 2), pl.ds(*span[k][i])]

    def r1(k, i, di, p):
        return out[k].at[other, di, p, pl.ds(*span[k][i])]

    def t2(k, i, d):
        return out[k].at[other, 3, 2, pl.ds(*cuts[k][i][int(d == 1)])]

    def r2(k, i, di, h):
        return out[k].at[other, 3, di, pl.ds(*cuts[k][i][h])]

    def remote(src, dst, send, recv, to):
        return pltpu.make_async_remote_copy(src, dst, send, recv, device_id=to, device_id_type=MESH)

    def local(src, dst, sem):
        return pltpu.make_async_copy(src, dst, sem)

    def most(k):
        return w[k].at[0, pl.ds(0, side * side - 1)]

    def pair_of_blocks(ref, k, i, p, h):
        lo, n = span[k][i]
        rows = pl.ds(lo, n)
        return ref.at[p, pl.ds(2 * h, 2), rows] if i == 0 else ref.at[pl.ds(2 * h, 2), p, rows]

    def row_of_blocks(ref, k, i):
        lo, n = span[k][i]
        rows = pl.ds(lo, n)
        return ref.at[pos[0], :, rows] if i == 0 else ref.at[:, pos[1], rows]

    pieces = [(i, d) for d in DIRS for i in CORES]

    def target(s, i, d):
        hf = 1 if d == 1 else 0
        return (at(pos[i] + 2), hf) if s == 0 else (at(pos[i] + d), 1 - hf if s == 1 else hf)

    def pair_copy(k, j):
        if j < 12:
            i, d = pieces[j % 4]
            p, h = target(j // 4, i, d)
            view = functools.partial(pair_of_blocks, k=k, i=i, p=p, h=h)
        else:
            view = functools.partial(row_of_blocks, k=k, i=j - 12)
        return remote(view(g[k].at[other]), view(land(k, other)), s_pair.at[k], r_pair.at[k, j], partner)

    quarters = [(b, h) for b in CORES for h in CORES]

    def quarter(ref, i, d, b, h):
        p, half = target(0, i, d)
        rows = pl.ds(*cuts[0][i][h])
        return ref.at[p, 2 * half + b, rows] if i == 0 else ref.at[2 * half + b, p, rows]

    def first_pair(i, d, b, h):
        return remote(quarter(g[0].at[other], i, d, b, h), quarter(land(0, other), i, d, b, h), s_pair.at[0], r_first.at[0, i, DIRS.index(d), b, h], partner)

    def first_send(i, d, b, h):
        lo, n = cuts[0][i][h]
        dst = t1(0, i, DIRS.index(d)).at[b, pl.ds(lo - span[0][i][0], n)]
        return remote(quarter(land(0), i, d, b, h), dst, s_rs.at[0], r_first.at[1, i, DIRS.index(d), b, h], device(i, d))

    def stage_first():
        for b, h in quarters:
            for j, (i, d) in enumerate(pieces):
                if (b, h) == quarters[0]:
                    own1_copy(j).wait()
                first_pair(i, d, b, h).wait_recv()
                lo, n = cuts[0][i][h]
                sums = quarter(land(0), i, d, b, h)
                add_into(sums, n, [own1.at[j % SLOTS, b, pl.ds(lo - span[0][i][0], n)], sums])
                first_send(i, d, b, h).start()
        for n in range(SLOTS, 2 * SLOTS - 1):
            own1_copy(n).start()

    order1 = [(k, s, i, d) for k in WEIGHTS for s in range(3) for i, d in pieces]

    def own1_copy(n):
        k, s, i, d = order1[n]
        p, h = target(s, i, d)
        return local(pair_of_blocks(g[k].at[c], k, i, p, h), own1.at[n % SLOTS, :, pl.ds(0, span[k][i][1])], s_own1.at[n % SLOTS])

    def own2_copy(k, i):
        return local(row_of_blocks(g[k].at[c], k, i), own2.at[i, :, pl.ds(0, span[k][i][1])], s_own2.at[i])

    def p_copy(k, s, i, d):
        di = DIRS.index(d)
        p, h = target(s, i, d)
        dst = t1(k, i, di) if s == 0 else r1(k, i, di, pl.ds(2 * h, 2))
        return remote(pair_of_blocks(land(k), k, i, p, h), dst, s_rs.at[k], r_p.at[k, s, i, di], device(i, d))

    def stage_p(k, s):
        if k + s == 0:
            return stage_first()
        for j, (i, d) in enumerate(pieces):
            n = order1.index((k, s, i, d))
            if n + SLOTS - 1 < len(order1):
                own1_copy(n + SLOTS - 1).start()
            own1_copy(n).wait()
            pair_copy(k, s * 4 + j).wait_recv()
            if s == 2 and k == 0:
                for b, h in quarters:
                    first_send(i, d, b, h).wait_recv()
            elif s == 2:
                p_copy(k, 0, i, d).wait_recv()
            p, h = target(s, i, d)
            sums = pair_of_blocks(land(k), k, i, p, h)
            for b in CORES:
                terms = [own1.at[n % SLOTS, b], sums.at[b]]
                if s == 2:
                    terms.append(t1(k, i, DIRS.index(d)).at[b])
                add_into(sums.at[b], span[k][i][1], terms)
            p_copy(k, s, i, d).start()

    def q_target(s, i, d):
        hf = 1 if d == 1 else 0
        p = pos[1 - i]
        return (at(p + 2), hf) if s == 0 else (at(p + d), 1 - hf if s == 1 else hf)

    def q_rows(ref, k, i, p, h):
        lo, n = cuts[k][i][h]
        return (ref.at[pos[0], p] if i == 0 else ref.at[p, pos[1]]).at[pl.ds(lo, n)]

    def q_copy(k, s, i, d):
        di = DIRS.index(d)
        p, h = q_target(s, i, d)
        dst = t2(k, i, d) if s == 0 else r2(k, i, di, h)
        return remote(q_rows(land(k), k, i, p, h), dst, s_rs.at[k], r_q.at[k, s, i, di], device(1 - i, d))

    def q_terms(k, i, p, h):
        off, n = cuts[k][i][h][0] - span[k][i][0], cuts[k][i][h][1]
        rows = pl.ds(off, n)
        return [own2.at[i, p, rows], q_rows(land(k), k, i, p, h)] + [r1(k, i, di, p).at[rows] for di in CORES]

    def stage_q(k, s):
        if s == 0:
            for i in CORES:
                own2_copy(k, i).wait()
                pair_copy(k, 12 + i).wait_recv()
            for i, d in pieces:
                p_copy(k, 1, i, d).wait_recv()
                p_copy(k, 2, i, d).wait_recv()
        for i, d in pieces:
            p, h = q_target(s, i, d)
            terms = q_terms(k, i, p, h)
            if s == 2:
                q_copy(k, 0, i, d).wait_recv()
                terms.append(t2(k, i, d))
            add_into(q_rows(land(k), k, i, p, h), cuts[k][i][h][1], terms)
            q_copy(k, s, i, d).start()

    def moment_refs(k):
        return m_out[max(k, IN_HBM)], v_out[max(k, IN_HBM)]

    def step_loads(k):
        new_m, new_v = moment_refs(k)
        return [local(w[k].at[:, x * side + y], w_raw, s_in.at[0]), local(m[k], new_m, s_in.at[1]), local(v[k], new_v, s_in.at[2])]

    def step_stores(k):
        if k >= IN_HBM:
            return []
        new_m, new_v = moment_refs(k)
        return [local(new_m, m_out[k], s_out.at[0]), local(new_v, v_out[k], s_out.at[1])]

    def own_rows(k, core):
        rows, lanes = forms[k]
        if rows % TILE == 0:
            return core * (rows * lanes), rows * lanes
        return core * (rows // TILE * TILE * lanes), (rows // TILE + 1) * TILE * lanes

    def grad_copy(k):
        lo, n = own_rows(k, other)
        rows = pl.ds(pl.multiple_of(lo, 8), n)
        return remote(grad.at[rows], grad_p.at[rows], s_grad.at[k], r_grad.at[k], partner)

    def x_copies(k):
        rows, lanes = forms[k]
        lo, n = own_rows(k, c)
        if rows % TILE == 0:
            mine = pl.ds(pl.multiple_of(lo, 8), n)
            return [remote(w_all.at[other, mine], w_all.at[other, mine], s_x.at[k, 0], r_x.at[k, 0], partner)]
        tile = TILE * lanes
        mine = pl.ds(pl.multiple_of(c * (n - 2 * tile + 2 * tile), 8), n - tile)
        middle = pl.ds(n - tile, tile)
        return [
            remote(w_all.at[other, mine], w_all.at[other, mine], s_x.at[k, 0], r_x.at[k, 0], partner),
            remote(w_all.at[other, middle], shared, s_x.at[k, 1], r_x.at[k, 1], partner),
        ]

    def take_step(k):
        rows, lanes = forms[k]

        def update(core):
            grads = (grad, grad_p) if core == 0 else (grad_p, grad)
            m_ref, v_ref = moment_refs(k)

            def one(layer, at_w, at_m):
                new_w, new_m, new_v = moments(w_all[layer, at_w, :], m_ref[at_m, :], v_ref[at_m, :], grads[layer][at_w, :])
                w_all[layer, at_w, :] = new_w
                m_ref[at_m, :] = new_m
                v_ref[at_m, :] = new_v

            if rows % TILE == 0:
                size = rows * lanes
                chunk = 8 * (rows // TILE)

                def body(n, _):
                    for layer in CORES:
                        one(layer, pl.ds(pl.multiple_of(core * size + n * chunk, 8), chunk), pl.ds(pl.multiple_of(layer * size + n * chunk, 8), chunk))
                    return 0

                lax.fori_loop(0, lanes, body, 0)
            else:
                first, last = core * rows, (core + 1) * rows
                parts = []
                r = first
                while r < last:
                    n = min(8 - r % 8, last - r)
                    parts.append((r, n))
                    r += n

                def body(lane, _):
                    for layer in CORES:
                        for r, n in parts:
                            one(layer, pl.ds((r // TILE * lanes + lane) * 8 + r % 8, n), pl.ds((r - first) * 2 * lanes + lane * 2 + layer, n, stride=2 * lanes))
                    return 0

                lax.fori_loop(0, lanes, body, 0)

        for core in CORES:
            pl.when(c == core)(functools.partial(update, core))

    def stage_step(k):
        loads = step_loads(k)
        loads[0].wait()
        for layer in CORES:

            def widen(start, size, layer=layer):
                w_all[layer, pl.ds(start, size), :] = w_raw[layer, pl.ds(start, size), :].astype(F32)

            loop(block, widen)
        for i, d in pieces:
            q_copy(k, 1, i, d).wait_recv()
            q_copy(k, 2, i, d).wait_recv()
        for i in CORES:
            for h in CORES:
                lo, n = cuts[k][i][h]
                terms = q_terms(k, i, pos[1 - i], h) + [r2(k, i, di, h) for di in CORES]
                add_into(grad.at[pl.ds(lo, n)], n, terms, F32)
        grad_copy(k).start()
        local(most(k), most(k), s_rs.at[k]).wait()
        for to in neighbours:
            pl.semaphore_signal(free.at[k], inc=1, device_id=to, device_id_type=MESH)
        loads[1].wait()
        loads[2].wait()
        grad_copy(k).wait_recv()
        take_step(k)
        for copy in step_stores(k):
            copy.start()
        swaps = x_copies(k)
        for copy in swaps:
            copy.start()
        for copy in swaps:
            copy.wait()
        rows, lanes = forms[k]
        if rows % TILE:
            tile = TILE * lanes
            start = rows // TILE * tile

            def merge(n, _):
                here = pl.ds(pl.multiple_of(start + n * 8, 8), 8)
                theirs = shared[pl.ds(pl.multiple_of(n * 8, 8), 8), :]
                mine = w_all[c, here, :]
                low = lax.broadcasted_iota(jnp.int32, theirs.shape, 0) < rows % TILE
                w_all[c, here, :] = jnp.where(low == (c == 0), mine, theirs)
                return 0

            lax.fori_loop(0, lanes, merge, 0)

        def narrow(start, size):
            out[k][c, x, y, pl.ds(start, size), :] = w_all[c, pl.ds(start, size), :].astype(BF16)

        loop(block, narrow)
        grad_copy(k).wait_send()
        for copy in step_stores(k):
            copy.wait()

    def place(i, first, second):
        return (second, first) if i == 0 else (first, second)

    def rows_of(k, i, h):
        return pl.ds(*(span[k][i] if h is None else cuts[k][i][h]))

    def ag_copy(k, i, along, d, first, second, h, event):
        dst = out[k].at[c, *place(i, first, second), rows_of(k, i, h)]
        return remote(dst, dst, s_ag.at[k], r_ag.at[k, i, event], device(1 - i if along == 0 else i, d))

    def fan(k, i, first, second, h):
        there = out[k].at[c, *place(i, first, second), rows_of(k, i, h)]
        remote(there, there, s_fan.at[k], r_fan.at[k], partner).start()

    def arrived(k, i, first, second, h, event):
        ag_copy(k, i, 0, 1, first, second, h, event).wait_recv()

    def ag_own(k):
        src = out[k].at[c, x, y]
        pl.semaphore_wait(free.at[k], len(neighbours))
        for i in CORES:
            f, s = pos[1 - i], pos[i]
            for di, d in enumerate(DIRS):
                ag_copy(k, i, 0, d, f, s, None, di).start()
            for di, d in enumerate(DIRS):
                ag_copy(k, i, 1, d, f, s, None, 4 + 5 * di).start()
        remote(src, src, s_fan.at[k], r_fan.at[k], partner).start()

    def ag_near(k):
        for di, d in enumerate(DIRS):
            for i in CORES:
                f, s = pos[1 - i], pos[i]
                from_ = at(f - d)
                arrived(k, i, from_, s, None, di)
                ag_copy(k, i, 0, d, from_, s, 1 - di, 2 + di).start()
                for d2i, d2 in enumerate(DIRS):
                    ag_copy(k, i, 1, d2, from_, s, None, 4 + 5 * d2i + 1 + di).start()
                fan(k, i, from_, s, None)

    def ag_far(k):
        for di, d in enumerate(DIRS):
            for i in CORES:
                f, s = pos[1 - i], pos[i]
                arrived(k, i, at(f + 2), s, 1 - di, 2 + di)
                for d2i, d2 in enumerate(DIRS):
                    ag_copy(k, i, 1, d2, at(f + 2), s, 1 - di, 4 + 5 * d2i + 3 + 1 - di).start()
                fan(k, i, at(f + 2), s, 1 - di)

    kinds = ((0, None, 0, 14), (-1, None, 0, 15), (1, None, 1, 16), (2, 0, 1, 17), (2, 1, 1, 18))

    def ag_second(k, n):
        rel, h, onward, event = kinds[n]
        for di, d in enumerate(DIRS):
            for i in CORES:
                f, s = pos[1 - i], pos[i]
                first, second = at(f + rel), at(s - d)
                arrived(k, i, first, second, h, 4 + 5 * di + n)
                if di == onward:
                    ag_copy(k, i, 1, d, first, second, h, event).start()
                fan(k, i, first, second, h)

    def ag_last(k, n):
        rel, h, _, event = kinds[n]
        for i in CORES:
            f, s = pos[1 - i], pos[i]
            arrived(k, i, at(f + rel), at(s + 2), h, event)
            fan(k, i, at(f + rel), at(s + 2), h)

    neighbours = [device(i, d) for i in CORES for d in DIRS]
    barrier = pltpu.get_barrier_semaphore()
    for to in (partner, *neighbours):
        pl.semaphore_signal(barrier, inc=1, device_id=to, device_id_type=MESH)
    for n in range(SLOTS):
        own1_copy(n).start()
    for i in CORES:
        own2_copy(0, i).start()
    pl.semaphore_wait(barrier, 1 + len(neighbours))
    for b, h in quarters:
        for i, d in pieces:
            first_pair(i, d, b, h).start()
    for k in WEIGHTS:
        for j in range(0 if k else len(pieces), 14):
            pair_copy(k, j).start()

    def stage_q_with_loads(k, s):
        if s == 0:
            for copy in step_loads(k):
                copy.start()
        stage_q(k, s)

    def stage_f(k):
        stage_step(k)
        if k + 1 < len(WEIGHTS):
            for i in CORES:
                own2_copy(k + 1, i).start()

    tasks = {"P": stage_p, "Q": stage_q_with_loads, "F": stage_f, "O": ag_own, "N": ag_near, "X": ag_far, "S": ag_second, "L": ag_last}
    for line in SCHEDULE:
        for task in line.split():
            tasks[task[0]](*(int(digit) for digit in task[1:]))

    for k in WEIGHTS:
        whole = land(k)
        local(whole, whole, s_pair.at[k]).wait()
        local(most(k), most(k), s_ag.at[k]).wait()
        local(whole, whole, s_fan.at[k]).wait()
        local(whole, whole, r_fan.at[k]).wait()


def deliver(*refs):
    n = (len(refs) - 4) // 2
    src, dst, (buffer, s_in, s_out, s_pass) = refs[:n], refs[n : 2 * n], refs[2 * n :]
    through = [j for j in range(len(WEIGHTS), n) if j % len(WEIGHTS) < IN_HBM]
    copies = []
    for at, j in enumerate(through):
        pltpu.make_async_copy(src[j], buffer.at[at], s_in.at[at]).start()
    for j in range(n):
        if j in through:
            continue
        if j < len(WEIGHTS):
            for core in CORES:
                for x in range(src[j].shape[1]):
                    pltpu.make_async_copy(src[j].at[core, x], dst[j].at[core, x], s_out.at[j]).start()
        else:
            pltpu.make_async_copy(src[j], dst[j], s_out.at[j]).start()
        copies.append(pltpu.make_async_copy(src[j], dst[j], s_out.at[j]))
    for at, j in enumerate(through):
        pltpu.make_async_copy(src[j], buffer.at[at], s_in.at[at]).wait()
        copies.append(pltpu.make_async_copy(buffer.at[at], dst[j], s_pass.at[at]))
        copies[-1].start()
    for copy in copies:
        copy.wait()


def tiles(a, chips):
    layers, rows, columns = a.shape
    a = a.reshape(layers, rows // TILE, TILE, columns // LANES, LANES).transpose(0, 1, 3, 2, 4)
    return a.reshape(layers, chips, -1, LANES)


def untiles(a, shape):
    layers, rows, columns = shape
    a = a.reshape(layers, rows // TILE, columns // LANES, TILE, LANES).transpose(0, 1, 3, 2, 4)
    return a.reshape(shape)


def moment_rows(a):
    layers, rows, columns = a.shape
    if rows % TILE == 0:
        return tiles(a, 1).reshape(-1, LANES)
    a = with_layout_constraint(a.reshape(layers, rows, columns // LANES, LANES), Layout(major_to_minor=(1, 2, 0, 3)))
    return a.transpose(1, 2, 0, 3).reshape(-1, LANES)


def moment_back(a, shape):
    layers, rows, columns = shape
    if rows % TILE == 0:
        return untiles(a, shape)
    return a.reshape(rows, columns // LANES, layers, 128).transpose(0, 2, 1, 3).reshape(rows, layers, columns).transpose(1, 0, 2)


def solution(mesh):
    n = mesh.shape["dp"]
    side = math.isqrt(n // 2)
    chips = side * side
    assert 2 * chips == n and side == 4

    def step(*arrays):
        terms, weights, m, v = (arrays[i : i + 3] for i in (0, 3, 6, 9))
        shapes, m_shapes = [a.shape for a in weights], [a.shape for a in m]
        block = math.prod(shapes[0][1:]) // chips // LANES
        forms = [(s[1], s[2] // LANES) for s in m_shapes]
        wide = max(sum(h[1] for h in i) for i in ranges(block, 0))
        odd = max([lanes * TILE for rows, lanes in forms if rows % TILE] + [8])
        split = (2, side, side, block, LANES)
        operands = (
            [tiles(t[0], chips).reshape(split) for t in terms] + [tiles(a, chips) for a in weights] + [moment_rows(a) for a in m + v]
        )
        dma = pltpu.SemaphoreType.DMA
        moment = jax.ShapeDtypeStruct(operands[6].shape, F32)
        anywhere, vmem = pl.BlockSpec(memory_space=pl.ANY), pl.BlockSpec(memory_space=pltpu.VMEM)
        made = pl.pallas_call(
            functools.partial(kernel, side, block, forms),
            out_shape=[pltpu.VMEM(split, BF16)] * 3 + ([moment] * IN_HBM + [pltpu.VMEM(moment.shape, F32)] * (3 - IN_HBM)) * 2,
            in_specs=[anywhere] * 12,
            out_specs=[vmem] * 3 + ([anywhere] * IN_HBM + [vmem] * (3 - IN_HBM)) * 2,
            scratch_shapes=[
                pltpu.VMEM((SLOTS, 2, wide, LANES), BF16),
                pltpu.VMEM((2, side, wide, LANES), BF16),
                pltpu.VMEM((block, LANES), F32),
                pltpu.VMEM((block, LANES), F32),
                pltpu.VMEM((2, block, LANES), BF16),
                pltpu.VMEM((2, block, LANES), F32),
                pltpu.VMEM((odd, LANES), F32),
                *(dma(shape) for shape in ((3,), (3, 14), (SLOTS,), (2,), (3,), (3, 3, 2, 2), (3, 3, 2, 2), (3,), (3,), (3,), (3, 2), (3, 2), (2,), (3,), (3, 2, 19), (3,), (3,), (2,) * 5)),
                pltpu.SemaphoreType.REGULAR((3,)),
            ],
            compiler_params=pltpu.CompilerParams(collective_id=0, has_side_effects=True, vmem_limit_bytes=VMEM_MAIN),
        )(*operands)
        made = [a if j >= 3 and j % 3 < IN_HBM else pltpu.with_memory_space_constraint(a, pltpu.VMEM) for j, a in enumerate(made)]
        results = pl.pallas_call(
            deliver,
            out_shape=[jax.ShapeDtypeStruct(a.shape, a.dtype) for a in made],
            in_specs=[anywhere] * 9,
            out_specs=[anywhere] * 9,
            scratch_shapes=[pltpu.VMEM((2 * IN_HBM, *moment.shape), F32), dma((2 * IN_HBM,)), dma((len(made),)), dma((2 * IN_HBM,))],
            compiler_params=pltpu.CompilerParams(vmem_limit_bytes=VMEM_MAIN),
        )(*made)
        new = [untiles(a, s) for a, s in zip(results[:3], shapes, strict=True)]
        return (*new, *(moment_back(a, s) for a, s in zip(results[3:], m_shapes * 2, strict=True)))

    all_of, cut = P(None, None, None), P(None, "dp", None)
    return jax.shard_map(
        step,
        mesh=mesh,
        in_specs=(P(("rep", "dp"), None, None, None),) * 3 + (all_of,) * 3 + (cut,) * 6,
        out_specs=(P("rep", None, None),) * 3 + (P("rep", "dp", None),) * 6,
        check_vma=False,
    )
```
